16 devices in a mesh: dp: 4 (over y, z, core), tp: 4 (over x).
Axes of the slice: x: 4, y: 2, z: 1, core: 2. Of those that a mesh axis runs over, the one named last changes fastest.
The devices are a block of a 4x4x8 slice.
Arguments:
- x: bfloat16 [8192, 3072], P('dp'), parts along dimension 0
- dy: bfloat16 [8192, 3072], P('dp'), parts along dimension 0
- gate: bfloat16 [8192, 8192], P('dp', 'tp'), parts along dimension 0
- up: bfloat16 [8192, 8192], P('dp', 'tp'), parts along dimension 0
- w_gate: bfloat16 [3072, 8192], P(None, 'tp')
- w_up: bfloat16 [3072, 8192], P(None, 'tp')
- w_down: bfloat16 [8192, 3072], P('tp')
Outputs:
- output 1: bfloat16 [8192, 3072], P('dp'), parts along dimension 0
- output 2: bfloat16 [12288, 8192], P('dp', 'tp'), parts along dimension 0
- output 3: bfloat16 [12288, 8192], P('dp', 'tp'), parts along dimension 0
- output 4: bfloat16 [32768, 3072], P(('dp', 'tp')), parts along dimension 0
There are 4 independent parts. The reference program is written for one: setup_inputs(seed, part) draws one part's arguments, and reference() takes and returns one part's arrays. A program takes and returns all parts, laid end to end along the dimension named above; an argument that names none is the same for every part.
All inputs are finite; a program needn't handle non-finite values.
Results may differ from the reference program's by a relative error of at most 0.012.
Values are sent between devices in bfloat16 or wider.
A program may use at most 768 MiB of HBM per device.

```python
import jax
import jax.numpy as jnp

ROWS = 2048
D = 3072
FF = 8192


def act(gate, up):
    return jax.nn.silu(gate) * up


def setup_inputs(seed: int = 0, part: int = 0) -> dict:
    kx, ky, ka, kb, kg, ku, kd = jax.random.split(jax.random.key(seed), 7)
    kx, ky, ka, kb = (jax.random.fold_in(k, part) for k in (kx, ky, ka, kb))
    drawn = {
        "x": jax.random.normal(kx, (ROWS, D), jnp.float32),
        "dy": jax.random.normal(ky, (ROWS, D), jnp.float32),
        "gate": jax.random.normal(ka, (ROWS, FF), jnp.float32),
        "up": jax.random.normal(kb, (ROWS, FF), jnp.float32),
        "w_gate": jax.random.normal(kg, (D, FF), jnp.float32) * D**-0.5,
        "w_up": jax.random.normal(ku, (D, FF), jnp.float32) * D**-0.5,
        "w_down": jax.random.normal(kd, (FF, D), jnp.float32) * FF**-0.5,
    }
    return {k: v.astype(jnp.bfloat16) for k, v in drawn.items()}


def reference(x, dy, gate, up, w_gate, w_up, w_down):
    hidden, back = jax.vjp(act, gate.astype(jnp.float32), up.astype(jnp.float32))
    d_hidden = jnp.dot(dy, w_down.T, preferred_element_type=jnp.float32)
    d_gate, d_up = (g.astype(jnp.bfloat16) for g in back(d_hidden))
    dx = jnp.dot(d_gate, w_gate.T, preferred_element_type=jnp.float32) + jnp.dot(d_up, w_up.T, preferred_element_type=jnp.float32)
    dw_gate = jnp.dot(x.T, d_gate, preferred_element_type=jnp.float32)
    dw_up = jnp.dot(x.T, d_up, preferred_element_type=jnp.float32)
    dw_down = jnp.dot(hidden.astype(jnp.bfloat16).T, dy, preferred_element_type=jnp.float32)
    return tuple(g.astype(jnp.bfloat16) for g in (dx, dw_gate, dw_up, dw_down))
```

```python
import functools

import jax
import jax.numpy as jnp
from jax import lax
from jax.experimental import pallas as pl
from jax.experimental.pallas import tpu as pltpu
from jax.sharding import PartitionSpec as P


BF16, F32 = jnp.bfloat16, jnp.float32
MESH = pl.DeviceIdType.MESH
VMEM_LIMIT = 66_000_000
UNIT = 128
FT = 512
DT = 512
MT, CT = 512, 512


def dot_nt(a, b):
    return lax.dot_general(a, b, (((1,), (1,)), ((), ())), preferred_element_type=F32)


def dot_tn(a, b):
    return lax.dot_general(a, b, (((0,), (0,)), ((), ())), preferred_element_type=F32)


def backward_reduce_scatter(
    n, axis,
    dy_ref, gate_ref, up_ref, wg_ref, wu_ref, wd_ref,
    dg_ref, du_ref, hid_ref, top_ref, bot_ref,
    dy_v, gate_v, up_v, dg_v, du_v, hid_v, wg_v, wu_v, wd_v, ring,
    in_sem, out_sem, w_sem, own_sem, send_sem, recv_sem,
):
    rows, width = dy_ref.shape
    hidden = gate_ref.shape[1]
    block = rows // n
    half = block // 2
    units = half // UNIT
    steps_f, pieces = hidden // FT, width // DT
    chunks = n * units

    me = lax.axis_index(axis)
    right, left = lax.rem(me + 1, n), lax.rem(me + n - 1, n)

    def first_rows(c):
        s, u = c // units, lax.rem(c, units)
        cw = lax.rem(me + 2 * n - 1 - s, n) * block + u * UNIT
        ccw = lax.rem(me + 1 + s, n) * block + half + u * UNIT
        return pl.multiple_of(cw, UNIT), pl.multiple_of(ccw, UNIT)

    def loads(c):
        slot = lax.rem(c, 2)
        out = []
        for d, start in enumerate(first_rows(c)):
            for k, (src, dst) in enumerate(((dy_ref, dy_v), (gate_ref, gate_v), (up_ref, up_v))):
                out.append(pltpu.make_async_copy(
                    src.at[pl.ds(start, UNIT)], dst.at[slot, pl.ds(d * UNIT, UNIT)], in_sem.at[slot, d, k]))
        return out

    def stores(c):
        out = []
        for d, start in enumerate(first_rows(c)):
            for k, (src, dst) in enumerate(((dg_v, dg_ref), (du_v, du_ref), (hid_v, hid_ref))):
                out.append(pltpu.make_async_copy(
                    src.at[pl.ds(d * UNIT, UNIT)], dst.at[pl.ds(start, UNIT)], out_sem.at[d, k]))
        return out

    def weights(g):
        if g < steps_f:
            part = pl.ds(g * FT, FT)
            return [pltpu.make_async_copy(wd_ref.at[part], wd_v.at[part], w_sem.at[g, 0])]
        part = pl.ds((g - steps_f) * DT, DT)
        return [pltpu.make_async_copy(src.at[part], dst.at[part], w_sem.at[g, k])
                for k, (src, dst) in enumerate(((wg_ref, wg_v), (wu_ref, wu_v)))]

    groups = steps_f + pieces

    def remote(d, s, u, h):
        return pltpu.make_async_remote_copy(
            src_ref=ring.at[d, s, u, h], dst_ref=ring.at[d, s + 1, u, h],
            send_sem=send_sem.at[d, s, u, h], recv_sem=recv_sem.at[d, s, u, h],
            device_id={axis: right if d == 0 else left}, device_id_type=MESH)

    def own(d, u, h):
        dst = (top_ref, bot_ref)[d]
        return pltpu.make_async_copy(
            ring.at[d, n - 1, u, h],
            dst.at[pl.ds(u * UNIT, UNIT), pl.ds(h * DT, DT)], own_sem.at[d, u, h])

    for copy in loads(0):
        copy.start()
    ahead = 3
    for g in range(ahead):
        for copy in weights(g):
            copy.start()

    barrier = pltpu.get_barrier_semaphore()
    for other in (left, right):
        pl.semaphore_signal(barrier, inc=1, device_id={axis: other}, device_id_type=MESH)
    ring[:, 0] = jnp.zeros_like(ring[:, 0])
    pl.semaphore_wait(barrier, 2)

    @pl.loop(0, chunks)
    def _(c):
        s, u = c // units, lax.rem(c, units)
        slot = lax.rem(c, 2)

        @pl.when(c + 1 < chunks)
        def _():
            for copy in loads(c + 1):
                copy.start()

        for copy in loads(c):
            copy.wait()

        @pl.when(c > 0)
        def _():
            for copy in stores(c - 1):
                copy.wait()

        def weights_here(g):
            @pl.when(c == 0)
            def _():
                for copy in weights(g):
                    copy.wait()
                if g + ahead < groups:
                    for copy in weights(g + ahead):
                        copy.start()

        for f in range(steps_f):
            weights_here(f)
            cols = pl.ds(f * FT, FT)
            dh = dot_nt(dy_v[slot], wd_v[cols, :])
            gate = gate_v[slot, :, cols].astype(F32)
            up = up_v[slot, :, cols].astype(F32)
            sig = jax.nn.sigmoid(gate)
            act = gate * sig
            hid_v[:, cols] = (act * up).astype(BF16)
            du_v[:, cols] = (dh * act).astype(BF16)
            dg_v[:, cols] = (dh * up * (sig + act * (1.0 - sig))).astype(BF16)

        for copy in stores(c):
            copy.start()

        for h in range(pieces):
            weights_here(steps_f + h)

            @pl.when(s > 0)
            def _():
                for d in range(2):
                    remote(d, s - 1, u, h).wait_recv()

            cols = pl.ds(h * DT, DT)
            term = dot_nt(dg_v[...], wg_v[cols, :]) + dot_nt(du_v[...], wu_v[cols, :])
            for d in range(2):
                ring[d, s, u, h] = (ring[d, s, u, h].astype(F32) + term[d * UNIT:(d + 1) * UNIT]).astype(BF16)

            @pl.when(s < n - 1)
            def _():
                for d in range(2):
                    remote(d, s, u, h).start()

            @pl.when(s == n - 1)
            def _():
                for d in range(2):
                    own(d, u, h).start()

    for copy in stores(chunks - 1):
        copy.wait()

    @pl.loop(0, units)
    def _(u):
        for d in range(2):
            for h in range(pieces):
                own(d, u, h).wait()

    @pl.loop(0, (n - 1) * units)
    def _(c):
        for d in range(2):
            for h in range(pieces):
                remote(d, c // units, lax.rem(c, units), h).wait_send()


def reduce_scatter_call(n, axis, dy, gate, up, wg, wu, wd):
    rows, width = dy.shape
    hidden = gate.shape[1]
    half = rows // n // 2
    units, pieces, groups = half // UNIT, width // DT, hidden // FT + width // DT
    flat = lambda *shape: jax.ShapeDtypeStruct(shape, BF16)
    any_ = pl.BlockSpec(memory_space=pl.ANY)
    dma = pltpu.SemaphoreType.DMA
    return pl.pallas_call(
        functools.partial(backward_reduce_scatter, n, axis),
        out_shape=(flat(rows, hidden), flat(rows, hidden), flat(rows, hidden), flat(half, width), flat(half, width)),
        in_specs=[any_] * 6,
        out_specs=(any_,) * 5,
        scratch_shapes=[
            pltpu.VMEM((2, 2 * UNIT, width), BF16),
            pltpu.VMEM((2, 2 * UNIT, hidden), BF16),
            pltpu.VMEM((2, 2 * UNIT, hidden), BF16),
            pltpu.VMEM((2 * UNIT, hidden), BF16),
            pltpu.VMEM((2 * UNIT, hidden), BF16),
            pltpu.VMEM((2 * UNIT, hidden), BF16),
            pltpu.VMEM((width, hidden), BF16),
            pltpu.VMEM((width, hidden), BF16),
            pltpu.VMEM((hidden, width), BF16),
            pltpu.VMEM((2, n, units, pieces, UNIT, DT), BF16),
            dma((2, 2, 3)), dma((2, 3)), dma((groups, 2)), dma((2, units, pieces)),
            dma((2, n - 1, units, pieces)), dma((2, n - 1, units, pieces)),
        ],
        compiler_params=pltpu.CompilerParams(
            collective_id=0, has_side_effects=True, vmem_limit_bytes=VMEM_LIMIT),
        cost_estimate=pl.CostEstimate(
            flops=6 * rows * width * hidden, transcendentals=rows * hidden,
            bytes_accessed=2 * (rows * width + 5 * rows * hidden + 3 * width * hidden)),
        name="dx_reduce_scatter",
    )(dy, gate, up, wg, wu, wd)


def copies(n, axis, shifts, srcs, out_ref, buf, in_sem, out_sem):
    half = buf.shape[1]
    me = lax.axis_index(axis)
    ins, outs = [], []
    for k, (shift, low) in enumerate(shifts):
        start = pl.multiple_of((2 * lax.rem(me + shift, n) + low) * half, half)
        ins.append(pltpu.make_async_copy(srcs[k], buf.at[k], in_sem.at[k]))
        outs.append(pltpu.make_async_copy(buf.at[k], out_ref.at[pl.ds(start, half)], out_sem.at[k]))
    return ins, outs


def dw_body(n, axis, shifts, a_ref, b_ref, *refs):
    count = len(shifts)
    srcs = refs[:count]
    o_ref, dx_ref, b_v, buf, b_sem, in_sem, out_sem = refs[-7:]
    cols = b_ref.shape[1]
    parts = cols // CT
    i, last = pl.program_id(0), pl.num_programs(0) - 1
    ins, outs = copies(n, axis, shifts, srcs, dx_ref, buf, in_sem, out_sem)
    loads = [pltpu.make_async_copy(b_ref.at[:, pl.ds(j * CT, CT)], b_v.at[:, pl.ds(j * CT, CT)], b_sem.at[j])
             for j in range(parts)]

    @pl.when(i == 0)
    def _():
        loads[0].start()
        loads[1].start()

    @pl.when(i == 1)
    def _():
        for copy in ins:
            copy.start()

    @pl.when(i == 2)
    def _():
        for copy in ins:
            copy.wait()
        for copy in outs:
            copy.start()

    def column(j):
        at = pl.ds(j * CT, CT)
        o_ref[:, at] = dot_tn(a_ref[...], b_v[:, at]).astype(BF16)

    @pl.when(i == 0)
    def _():
        for j in range(parts):
            loads[j].wait()
            if j + 2 < parts:
                loads[j + 2].start()
            column(j)

    @pl.when(i > 0)
    def _():
        for j in range(parts):
            column(j)

    @pl.when(i == last)
    def _():
        for copy in outs:
            copy.wait()


def dw_call(n, axis, a, b, shifts, pieces, dx):
    rows, m = a.shape
    cols = b.shape[1]
    half, width = pieces[0].shape
    count = len(pieces)
    any_ = pl.BlockSpec(memory_space=pl.ANY)
    extra = () if dx is None else (dx,)
    dma = pltpu.SemaphoreType.DMA
    return pl.pallas_call(
        functools.partial(dw_body, n, axis, shifts),
        grid=(m // MT,),
        out_shape=(jax.ShapeDtypeStruct((m, cols), BF16), jax.ShapeDtypeStruct((rows, width), BF16)),
        in_specs=[pl.BlockSpec((rows, MT), lambda i: (0, i)), any_] + [any_] * (count + len(extra)),
        out_specs=(pl.BlockSpec((MT, cols), lambda i: (i, 0)), any_),
        scratch_shapes=[pltpu.VMEM((rows, cols), BF16), pltpu.VMEM((count, half, width), BF16),
                        dma((cols // CT,)), dma((count,)), dma((count,))],
        input_output_aliases={2 + count: 1} if extra else {},
        compiler_params=pltpu.CompilerParams(vmem_limit_bytes=VMEM_LIMIT),
        cost_estimate=pl.CostEstimate(
            flops=2 * rows * m * cols, transcendentals=0,
            bytes_accessed=2 * (rows * m + rows * cols + m * cols)),
    )(a, b, *pieces, *extra)


def place_body(n, axis, shifts, *refs):
    count = len(shifts)
    out_ref, buf, in_sem, out_sem = refs[count + 1:]
    ins, outs = copies(n, axis, shifts, refs[:count], out_ref, buf, in_sem, out_sem)
    for copy in ins:
        copy.start()
    for i, o in zip(ins, outs):
        i.wait()
        o.start()
    for copy in outs:
        copy.wait()


def place_call(n, axis, shifts, pieces, dx):
    any_ = pl.BlockSpec(memory_space=pl.ANY)
    half, width = pieces[0].shape
    count = len(pieces)
    dma = pltpu.SemaphoreType.DMA
    return pl.pallas_call(
        functools.partial(place_body, n, axis, shifts),
        out_shape=jax.ShapeDtypeStruct(dx.shape, BF16),
        in_specs=[any_] * (count + 1),
        out_specs=any_,
        scratch_shapes=[pltpu.VMEM((count, half, width), BF16), dma((count,)), dma((count,))],
        input_output_aliases={count: 0},
        compiler_params=pltpu.CompilerParams(vmem_limit_bytes=VMEM_LIMIT),
        cost_estimate=pl.CostEstimate(flops=200 * count * half * width, transcendentals=0, bytes_accessed=4 * count * half * width),
    )(*pieces, dx)


def solution(mesh):
    axis = "tp"
    n = mesh.shape[axis]
    to_right = [(i, (i + 1) % n) for i in range(n)]
    to_left = [(i, (i + n - 1) % n) for i in range(n)]

    def send(part, pairs):
        return lax.ppermute(part, axis, pairs)

    def step(x, dy, gate, up, w_gate, w_up, w_down):
        d_gate, d_up, hid, top, bot = reduce_scatter_call(n, axis, dy, gate, up, w_gate, w_up, w_down)
        left_top = send(top, to_right)
        right_bot = send(bot, to_left)
        left_bot = send(bot, to_right)
        right_top = send(top, to_left)
        dw_gate, dx = dw_call(n, axis, x, d_gate, ((0, 0), (0, 1)), (top, bot), None)
        far_top = send(left_top, to_right)
        far_bot = send(right_bot, to_left)
        dw_up, dx = dw_call(n, axis, x, d_up, ((n - 1, 0), (1, 1)), (left_top, right_bot), dx)
        dw_down, dx = dw_call(n, axis, hid, dy, ((n - 1, 1), (1, 0)), (left_bot, right_top), dx)
        dx = place_call(n, axis, ((2, 0), (2, 1)), (far_top, far_bot), dx)
        return dx, dw_gate, dw_up, dw_down

    tokens, columns, rows = P("dp", None), P(None, "tp"), P("tp", None)
    return jax.shard_map(
        step,
        mesh=mesh,
        in_specs=(tokens, tokens, P("dp", "tp"), P("dp", "tp"), columns, columns, rows),
        out_specs=(tokens, P("dp", "tp"), P("dp", "tp"), P(("dp", "tp"), None)),
        check_vma=False,
    )
```
